32 devices in a mesh: level: 4 (over y, core), blk: 8 (over z, x).
Axes of the slice: x: 2, y: 2, z: 4, core: 2. Of those that a mesh axis runs over, the one named last changes fastest.
Arguments:
- right_sides: bfloat16 [4, 8, 1024, 384], P('level', 'blk'), may hold values from -6 to 6
- diag_inverse: bfloat16 [4, 8, 1, 1024, 1024], P('level', 'blk'), may hold values from -0.1875 to 0.1875
- compress_basis: bfloat16 [4, 8, 1024, 256], P('level', 'blk'), may hold values from -0.1875 to 0.1875
- expand_basis: bfloat16 [4, 8, 1024, 256], P('level', 'blk'), may hold values from -0.125 to 0.125
- target_ranks: int32 [4, 8], P('level', 'blk'), may hold values from 32 to 256
- coupling: int32 [4, 8, 4, 8], replicated, may hold values 0 or 1
- section_order: int32 [4], replicated, may hold values from 0 to 3, each once
Outputs:
- solved: bfloat16 [4, 8, 1024, 384], P('level', 'blk')
The draws below stay inside these ranges and needn't reach their ends.
All inputs are finite; a program needn't handle non-finite values.
Results may differ from the reference program's by a relative error of at most 0.015.
Values may be sent and summed in bfloat16 or wider, within the bound.
No kernel may reach another device: no remote copies, remote signals or barrier semaphores. Data moves between devices by JAX's collectives and lax.ppermute only.
A program may use at most 128 MiB of HBM per device.

```python
import jax
import jax.numpy as jnp
from jax import lax

B = 1024
BLK_DEV = 1
KMAX = 256
RHS = 384
SEG = 1024
LEVELS = 4
BLOCKS = 8
N_LEVEL = 4
N_BLK = 8


def touch_ends(entries, own_key, smallest, largest):
    spot = [jax.random.randint(jax.random.fold_in(own_key, axis), (), 0, length) for axis, length in enumerate(entries.shape)]
    main_axis = entries.shape.index(max(entries.shape))
    neighbour = spot[:main_axis] + [(spot[main_axis] + 1) % entries.shape[main_axis]] + spot[main_axis + 1:]
    return entries.at[tuple(spot)].set(smallest).at[tuple(neighbour)].set(largest)


def level_of(stream_key, dims, split, low, high):
    level, own = 1.0, jax.random.fold_in(stream_key, 6)
    for position, blocks in split:
        heights = jnp.exp(jax.random.uniform(jax.random.fold_in(own, position), (blocks,), jnp.float32, low / len(split), high / len(split)))
        level = level * jnp.repeat(heights, dims[position] // blocks).reshape([-1 if axis == position else 1 for axis in range(len(dims))])
    return level


def noise(own_key, dims, width, limit, pieces=(), held_as=jnp.bfloat16):
    factor_of = level_of(own_key, dims, pieces, -0.22, 0.18) if pieces else 1.0
    drawn = jax.random.normal(own_key, dims, jnp.float32) * width * factor_of
    return jnp.minimum(jnp.maximum(drawn, -limit), limit).astype(held_as)


def setup_inputs(seed: int = 0) -> dict:
    key_of = jax.random.split(jax.random.key(seed), 8)
    right_sides = noise(key_of[0], (LEVELS, BLOCKS, SEG, RHS), 1.0, 6.0, ((0, 4), (1, 8)))
    diag_inverse = noise(key_of[1], (LEVELS, BLOCKS, BLK_DEV, B, B), B ** -0.5, 0.1875, ((0, 4), (1, 8)))
    compress_basis = noise(key_of[2], (LEVELS, BLOCKS, SEG, KMAX), SEG ** -0.5, 0.1875, ((0, 4), (1, 8)))
    expand_basis = noise(key_of[3], (LEVELS, BLOCKS, SEG, KMAX), (KMAX * 8) ** -0.5, 0.125, ((0, 4), (1, 8)))
    target_ranks = touch_ends(jax.random.randint(key_of[4], (LEVELS, BLOCKS), KMAX // 8, KMAX + 1), jax.random.fold_in(key_of[4], 1), KMAX // 8, KMAX).astype(jnp.int32)
    coupling = touch_ends((jax.random.randint(key_of[5], (LEVELS, BLOCKS, LEVELS, BLOCKS), 0, 4) < 1).astype(jnp.int32), jax.random.fold_in(key_of[5], 1), 0, 1)
    section_order = jax.random.permutation(key_of[6], LEVELS).astype(jnp.int32)
    return {"right_sides": right_sides, "diag_inverse": diag_inverse, "compress_basis": compress_basis, "expand_basis": expand_basis, "target_ranks": target_ranks, "coupling": coupling, "section_order": section_order}


def reference(right_sides, diag_inverse, compress_basis, expand_basis, target_ranks, coupling, section_order):
    coef_all = jnp.zeros((N_LEVEL, N_BLK, KMAX, RHS), jnp.float32)
    solved = jnp.zeros((N_LEVEL, N_BLK, SEG, RHS), jnp.bfloat16)
    level_ids = jnp.arange(N_LEVEL, dtype=jnp.int32)
    for level_step in range(N_LEVEL):
        group_now = jnp.sum(jnp.where(section_order == level_step, level_ids, 0)).astype(jnp.int32)
        weights = lax.dynamic_index_in_dim(coupling, group_now, 0, keepdims=False).astype(jnp.float32)
        incoming = jnp.einsum('bhc,hckr->bkr', weights, coef_all, precision=lax.Precision.HIGHEST)
        incoming = lax.optimization_barrier(incoming.astype(jnp.bfloat16)).astype(jnp.float32)
        expand_now = lax.dynamic_index_in_dim(expand_basis, group_now, 0, keepdims=False).astype(jnp.float32)
        update = jnp.einsum('bsk,bkr->bsr', expand_now, incoming)
        sides_now = lax.dynamic_index_in_dim(right_sides, group_now, 0, keepdims=False).astype(jnp.float32)
        work_rows = (sides_now - update).astype(jnp.bfloat16).astype(jnp.float32)
        work_rows = work_rows.reshape(N_BLK, BLK_DEV, B, RHS)
        inverse_now = lax.dynamic_index_in_dim(diag_inverse, group_now, 0, keepdims=False).astype(jnp.float32)
        solved_rows = jnp.einsum('njab,njbr->njar', inverse_now, work_rows)
        solved_rows = solved_rows.astype(jnp.bfloat16).reshape(N_BLK, SEG, RHS)
        basis_now = lax.dynamic_index_in_dim(compress_basis, group_now, 0, keepdims=False).astype(jnp.float32)
        coef_new = jnp.einsum('nsk,nsr->nkr', basis_now, solved_rows.astype(jnp.float32))
        ranks_now = lax.dynamic_index_in_dim(target_ranks, group_now, 0, keepdims=False)
        rank_mask = jnp.arange(KMAX, dtype=jnp.int32)[None, :] < ranks_now[:, None]
        coef_new = jnp.where(rank_mask[:, :, None], coef_new, 0.0)
        coef_new = lax.optimization_barrier(coef_new.astype(jnp.bfloat16)).astype(jnp.float32)
        coef_all = lax.dynamic_update_index_in_dim(coef_all, coef_new, group_now, 0)
        solved = lax.dynamic_update_index_in_dim(solved, solved_rows, group_now, 0)
    return solved
```

```python
import functools

import jax
import jax.numpy as jnp
from jax import lax
from jax.experimental import pallas as pl
from jax.experimental.pallas import tpu as pltpu
from jax.sharding import Mesh, PartitionSpec as P


def x_size(mesh):
    blocks = mesh.shape["blk"]
    first = [getattr(d, "coords", None) for d in mesh.devices[0]]
    if any(c is None for c in first):
        return 2 if blocks % 2 == 0 else 1
    return len({c[0] for c in first})


def mid_kernel(step, zs, xs, order_ref, coup_ref, place_ref, *refs):
    my_z, my_x = place_ref[0], place_ref[1]
    pieces = [refs[h * zs : (h + 1) * zs] for h in range(step)]
    c0_ref = refs[step * zs]
    m_refs = refs[step * zs + 1 : step * zs + 1 + xs]
    inc_ref, out_ref = refs[-2:]
    group = order_ref[step]
    for mb in range(xs):
        xb = my_x ^ mb
        inc = mix(step, zs, xs, order_ref, coup_ref, pieces, group, my_z, xb)
        inc = inc.astype(jnp.bfloat16)
        inc_ref[xb] = inc
        delta = jnp.dot(inc, m_refs[mb][...], preferred_element_type=jnp.float32)
        out_ref[xb] = (c0_ref[group, xb].astype(jnp.float32) - delta).astype(jnp.bfloat16)


def mix(step, zs, xs, order_ref, coup_ref, pieces, group, my_z, xb):
    total = None
    for h in range(step):
        for m in range(zs):
            for xc in range(xs):
                w = coup_ref[group, my_z * xs + xb, order_ref[h] * (zs * xs) + (my_z ^ m) * xs + xc]
                term = w.astype(jnp.float32) * pieces[h][m][xc].astype(jnp.float32)
                total = term if total is None else total + term
    return total


def last_kernel(levels, zs, xs, order_ref, coup_ref, place_ref, *refs):
    my_z = place_ref[0]
    step = levels - 1
    pieces = [refs[h * zs : (h + 1) * zs] for h in range(step)]
    inc_refs = refs[step * zs : -1]
    out_ref = refs[-1]
    out_ref[order_ref[0]] = jnp.zeros(out_ref.shape[1:], out_ref.dtype)
    for h in range(1, step):
        out_ref[order_ref[h]] = inc_refs[h - 1][...]
    group = order_ref[step]
    for xb in range(xs):
        inc = mix(step, zs, xs, order_ref, coup_ref, pieces, group, my_z, xb)
        out_ref[group, xb] = inc.astype(jnp.bfloat16)


def per_device(zs, xs, sides, inverse, compress, expand, ranks, coupling, section_order):
    levels = lax.axis_size("level")
    blocks = zs * xs
    my_z, my_x = lax.axis_index("z"), lax.axis_index("x")
    sides, expand, basis = sides[0, 0], expand[0, 0], compress[0, 0]
    inverse = inverse[0, 0]
    subs, rows = inverse.shape[0], inverse.shape[1]
    rank_cap, width = basis.shape[1], sides.shape[1]
    cols = width // (levels * xs)
    tn = (((0,), (0,)), ((), ()))
    bf16, f32 = jnp.bfloat16, jnp.float32

    kept = jnp.arange(rank_cap, dtype=jnp.int32)[None, :] < ranks[0, 0]
    reduced = jnp.einsum(
        "jab,jak->jbk", inverse, basis.reshape(subs, rows, rank_cap), preferred_element_type=f32
    )
    reduced = jnp.where(kept, reduced.reshape(subs * rows, rank_cap), 0.0).astype(bf16)
    c0 = lax.dot_general(sides, reduced, tn, preferred_element_type=f32).astype(bf16)
    m_t = lax.dot_general(expand, reduced, tn, preferred_element_type=f32).astype(bf16)

    level_ids = jnp.arange(levels, dtype=jnp.int32)
    order = jnp.sum(
        jnp.where(section_order[None, :] == level_ids[:, None], level_ids[None, :], 0), axis=1
    ).astype(jnp.int32)
    place = jnp.stack([my_z, my_x]).astype(jnp.int32)
    coup = coupling.reshape(levels, blocks, levels * blocks)

    m_all = lax.all_gather(m_t, "level", axis=0)
    m_mid = jnp.stack(
        [lax.dynamic_index_in_dim(m_all, order[s], 0, keepdims=False) for s in range(1, levels - 1)]
    )
    m_parts = [m_mid] + [
        lax.ppermute(m_mid, "x", [(i, i ^ m) for i in range(xs)]) for m in range(1, xs)
    ]
    c0_all = lax.all_to_all(c0, ("level", "x"), 0, 0, tiled=True)
    c0_all = c0_all.reshape(levels, xs, cols, rank_cap)

    smem = pl.BlockSpec(memory_space=pltpu.SMEM)
    vmem = pl.BlockSpec(memory_space=pltpu.VMEM)
    share = jax.ShapeDtypeStruct((xs, cols, rank_cap), bf16)

    def exchange(part):
        return [part] + [
            lax.ppermute(part, "z", [(i, i ^ m) for i in range(zs)]) for m in range(1, zs)
        ]

    solved = lax.dynamic_index_in_dim(c0_all, order[0], 0, keepdims=False)
    pieces, incs = [], []
    for step in range(1, levels):
        pieces += exchange(solved)
        if step < levels - 1:
            ms = [part[step - 1] for part in m_parts]
            n_in = len(pieces) + 1 + len(ms)
            inc, solved = pl.pallas_call(
                functools.partial(mid_kernel, step, zs, xs),
                in_specs=[smem] * 3 + [vmem] * n_in,
                out_specs=[vmem, vmem],
                out_shape=[share, share],
                name=f"section_{step}",
            )(order, coup, place, *pieces, c0_all, *ms)
            incs.append(inc)
    inc_all = pl.pallas_call(
        functools.partial(last_kernel, levels, zs, xs),
        in_specs=[smem] * 3 + [vmem] * (len(pieces) + len(incs)),
        out_specs=vmem,
        out_shape=jax.ShapeDtypeStruct((levels, xs, cols, rank_cap), bf16),
        name="last_sums",
    )(order, coup, place, *pieces, *incs)
    inc = lax.all_to_all(
        inc_all.reshape(levels * xs * cols, rank_cap), ("level", "x"), 0, 0, tiled=True
    )

    update = lax.dot_general(expand, inc, (((1,), (1,)), ((), ())), preferred_element_type=f32)
    work = (sides.astype(f32) - update).astype(bf16).reshape(subs, rows, width)
    result = jnp.einsum("jab,jbr->jar", inverse, work, preferred_element_type=f32)
    return result.astype(bf16).reshape(1, 1, subs * rows, width)


def solution(mesh):
    levels, blocks = mesh.shape["level"], mesh.shape["blk"]
    xs = x_size(mesh)
    zs = blocks // xs
    split = Mesh(mesh.devices.reshape(levels, zs, xs), ("level", "z", "x"))
    seg = P("level", ("z", "x"))
    return jax.shard_map(
        functools.partial(per_device, zs, xs),
        mesh=split,
        in_specs=(seg, seg, seg, seg, seg, P(), P()),
        out_specs=seg,
        check_vma=False,
    )
```

```python
import functools

import jax
import jax.numpy as jnp
from jax import lax
from jax.experimental import pallas as pl
from jax.experimental.pallas import tpu as pltpu
from jax.sharding import Mesh, PartitionSpec as P

BF16, F32 = jnp.bfloat16, jnp.float32
NN = (((1,), (0,)), ((), ()))
NT = (((1,), (1,)), ((), ()))
TN = (((0,), (0,)), ((), ()))
MIB = 1 << 20


def dot(a, b, dims):
    return lax.dot_general(a, b, dims, preferred_element_type=F32)


def x_size(mesh):
    blocks = mesh.shape["blk"]
    coords = [getattr(d, "coords", None) for d in mesh.devices[0]]
    if any(c is None for c in coords):
        return 2 if blocks % 2 == 0 else 1
    return len({c[0] for c in coords})


def call(kernel, outs, name, flops, nbytes, vmem, **kw):
    return pl.pallas_call(
        kernel,
        out_shape=outs,
        name=name,
        cost_estimate=pl.CostEstimate(flops=flops, bytes_accessed=nbytes, transcendentals=0),
        compiler_params=pltpu.CompilerParams(vmem_limit_bytes=vmem),
        **kw,
    )


def prep_kernel(chunk, rank_ref, c_hbm, d_hbm, r_hbm, e_hbm, out_ref, c, d, r, e, acc, sems):
    subs, rows = d_hbm.shape[0], d_hbm.shape[1]
    parts = rows // chunk
    copies = [pltpu.make_async_copy(c_hbm, c, sems.at[0])]
    for j in range(subs):
        for i in range(parts):
            at = pl.ds(i * chunk, chunk)
            copies.append(
                pltpu.make_async_copy(d_hbm.at[j, at], d.at[j, at], sems.at[1 + j * parts + i])
            )
    copies.append(pltpu.make_async_copy(r_hbm, r, sems.at[1 + subs * parts]))
    copies.append(pltpu.make_async_copy(e_hbm, e, sems.at[2 + subs * parts]))
    for copy in copies:
        copy.start()
    copies[0].wait()
    for j in range(subs):
        wide = pl.ds(j * rows, rows)
        for i in range(parts):
            copies[1 + j * parts + i].wait()
            part = dot(
                c[pl.ds(j * rows + i * chunk, chunk), :], d[j, pl.ds(i * chunk, chunk), :], TN
            )
            acc[:, wide] = part if i == 0 else acc[:, wide] + part
    a = acc[...].astype(BF16)
    kept = lax.broadcasted_iota(jnp.int32, (a.shape[0], 1), 0) < rank_ref[0, 0]
    copies[-2].wait()
    c0 = jnp.where(kept, dot(a, r[...], NN), 0.0).T.astype(BF16)
    copies[-1].wait()
    m = jnp.where(kept, dot(a, e[...], NN), 0.0).astype(BF16)
    levels, xs = out_ref.shape[0], out_ref.shape[1]
    cols, half = c0.shape[0] // (levels * xs), m.shape[0] // 2
    for level in range(levels):
        for x in range(xs):
            at = (level * xs + x) * cols
            out_ref[level, x, :cols] = c0[at : at + cols]
            out_ref[level, x, cols:] = m[level % 2 * half : (level % 2 + 1) * half]


def weights_kernel(zs, xs, levels, order_ref, coup_ref, w_ref, pick_ref):
    my_z = lax.axis_index("z")
    blocks = zs * xs
    row = 0
    for step in range(1, levels):
        for xb in range(xs):
            for h in range(step):
                for m in range(zs):
                    for xc in range(xs):
                        at = order_ref[h] * blocks + (my_z ^ m) * xs + xc
                        w = coup_ref[order_ref[step], my_z * xs + xb, at].astype(F32)
                        w_ref[pl.ds(row, 1), :] = jnp.full((1, w_ref.shape[1]), w, F32)
                        row += 1
    for step in range(levels):
        for g in range(levels):
            hit = (order_ref[step] == g).astype(F32)
            pick_ref[pl.ds(step * levels + g, 1), :] = jnp.full((1, w_ref.shape[1]), hit, F32)


def mix(first, step, zs, xs, w_ref, pieces, xb):
    row = first + xb * step * zs * xs
    total = None
    for h in range(step):
        for m in range(zs):
            for xc in range(xs):
                term = w_ref[pl.ds(row, 1), :] * pieces[h * zs + m][xc].astype(F32)
                total = term if total is None else total + term
                row += 1
    return total


def first_row(step, zs, xs):
    return xs * zs * xs * (step * (step - 1) // 2)


def mid_kernel(step, zs, xs, *refs):
    pieces = refs[: step * zs]
    w_ref, c0_ref, own_ref, other_ref, inc_ref, out_ref = refs[step * zs :]
    half = own_ref.shape[1]
    core = lax.rem(lax.axis_index("level"), 2)
    mine = pl.ds(pl.multiple_of(core * half, half), half)
    theirs = pl.ds(pl.multiple_of((1 - core) * half, half), half)
    for xb in range(xs):
        inc = mix(first_row(step, zs, xs), step, zs, xs, w_ref, pieces, xb).astype(BF16)
        inc_ref[xb] = inc
        out_ref[xb, :, mine] = (
            c0_ref[xb, :, mine].astype(F32) - dot(inc, own_ref[xb], NT)
        ).astype(BF16)
        out_ref[xb, :, theirs] = (
            c0_ref[xb, :, theirs].astype(F32) - dot(inc, other_ref[xb], NT)
        ).astype(BF16)


def last_kernel(levels, zs, xs, *refs):
    step = levels - 1
    pieces = refs[: step * zs]
    w_ref, pick_ref = refs[step * zs : step * zs + 2]
    inc_refs = refs[step * zs + 2 : -1]
    out_ref = refs[-1]
    for xb in range(xs):
        incs = [ref[xb].astype(F32) for ref in inc_refs]
        incs.append(mix(first_row(step, zs, xs), step, zs, xs, w_ref, pieces, xb))
        for g in range(levels):
            total = None
            for h in range(1, levels):
                term = pick_ref[pl.ds(h * levels + g, 1), :] * incs[h - 1]
                total = term if total is None else total + term
            out_ref[g, xb] = total.astype(BF16)


def full_kernel(d_hbm, r_hbm, e_hbm, dr_ref, de_ref, d, r, e, sems):
    copies = [
        pltpu.make_async_copy(r_hbm, r, sems.at[0]),
        pltpu.make_async_copy(e_hbm, e, sems.at[1]),
        pltpu.make_async_copy(d_hbm, d, sems.at[2]),
    ]
    for copy in copies:
        copy.start()
    for copy in copies:
        copy.wait()
    for j in range(d.shape[0]):
        at = pl.ds(j * d.shape[1], d.shape[1])
        dr_ref[at, :] = dot(d[j], r[at, :], NN)
        de_ref[at, :] = dot(d[j], e[at, :], NN).astype(BF16)


def final_kernel(tiles, inc_ref, dr_ref, de_ref, out_hbm, out, sems):
    tile = out.shape[0] // tiles
    copies = []
    for t in range(tiles):
        at = pl.ds(t * tile, tile)
        out[at, :] = (dr_ref[at, :] - dot(de_ref[at, :], inc_ref[...], NT)).astype(BF16)
        copies.append(pltpu.make_async_copy(out.at[at], out_hbm.at[at], sems.at[t]))
        copies[-1].start()
    for copy in copies:
        copy.wait()


def per_device(zs, xs, sides, inverse, compress, expand, ranks, coupling, section_order):
    levels = lax.axis_size("level")
    blocks = zs * xs
    sides, expand, basis, inverse = sides[0, 0], expand[0, 0], compress[0, 0], inverse[0, 0]
    subs, rows = inverse.shape[0], inverse.shape[1]
    seg, width = sides.shape
    rank_cap = basis.shape[1]
    cols = width // (levels * xs)
    half = rank_cap // 2
    smem = pl.BlockSpec(memory_space=pltpu.SMEM)
    vmem = pl.BlockSpec(memory_space=pltpu.VMEM)
    hbm = pl.BlockSpec(memory_space=pl.ANY)
    shape = jax.ShapeDtypeStruct

    chunk = rows // 4 if rows % 512 == 0 else rows
    n_copies = 3 + subs * (rows // chunk)
    payload = call(
        functools.partial(prep_kernel, chunk),
        shape((levels, xs, cols + half, rank_cap), BF16),
        "prep",
        2 * rank_cap * (seg * rows + seg * (width + rank_cap)),
        2 * (seg * (rows + width + 2 * rank_cap)),
        62 * MIB,
        in_specs=[smem] + [hbm] * 4,
        out_specs=vmem,
        scratch_shapes=[
            pltpu.VMEM(basis.shape, BF16),
            pltpu.VMEM(inverse.shape, BF16),
            pltpu.VMEM(sides.shape, BF16),
            pltpu.VMEM(expand.shape, BF16),
            pltpu.VMEM((rank_cap, seg), F32),
            pltpu.SemaphoreType.DMA((n_copies,)),
        ],
    )(ranks, basis, inverse, sides, expand)

    level_ids = jnp.arange(levels, dtype=jnp.int32)
    order = jnp.sum(
        jnp.where(section_order[None, :] == level_ids[:, None], level_ids[None, :], 0), axis=1
    ).astype(jnp.int32)

    shares = lax.all_to_all(
        payload.reshape(levels * xs * (cols + half), rank_cap), ("level", "x"), 0, 0, tiled=True
    ).reshape(levels, xs, cols + half, rank_cap)

    n_rows = first_row(levels, zs, xs)
    w_rows, picks = call(
        functools.partial(weights_kernel, zs, xs, levels),
        (shape((n_rows, rank_cap), F32), shape((levels * levels, rank_cap), F32)),
        "weights",
        1 << 20,
        4 * n_rows * rank_cap,
        4 * MIB,
        in_specs=[smem, smem],
        out_specs=(vmem, vmem),
    )(order, coupling.reshape(levels, blocks, levels * blocks))

    dr, de = call(
        full_kernel,
        (shape((seg, width), F32), shape((seg, rank_cap), BF16)),
        "full",
        2 * seg * rows * (width + rank_cap),
        2 * seg * (rows + 3 * width + 2 * rank_cap),
        62 * MIB,
        in_specs=[hbm] * 3,
        out_specs=(vmem, vmem),
        scratch_shapes=[
            pltpu.VMEM(inverse.shape, BF16),
            pltpu.VMEM(sides.shape, BF16),
            pltpu.VMEM(expand.shape, BF16),
            pltpu.SemaphoreType.DMA((3,)),
        ],
    )(inverse, sides, expand)

    shares, w_rows, picks, dr, de = lax.optimization_barrier((shares, w_rows, picks, dr, de))

    def part_of(step, start, size):
        zero = jnp.zeros((), jnp.int32)
        at = (order[step], zero, jnp.full((), start, jnp.int32), zero)
        return lax.dynamic_slice(shares, at, (1, xs, size, rank_cap))

    m_mine = jnp.concatenate([part_of(s, cols, half) for s in range(1, levels - 1)])
    m_other = lax.ppermute(m_mine, "level", [(i, i ^ 1) for i in range(levels)])

    def exchange(part):
        return [part] + [
            lax.ppermute(part, "z", [(i, i ^ m) for i in range(zs)]) for m in range(1, zs)
        ]

    share = shape((xs, cols, rank_cap), BF16)
    size = 2 * xs * cols * rank_cap
    solved = part_of(0, 0, cols)[0]
    pieces, incs = [], []
    for step in range(1, levels):
        pieces += exchange(solved)
        flops = 2 * step * zs * xs * size
        if step < levels - 1:
            inc, solved = call(
                functools.partial(mid_kernel, step, zs, xs),
                (share, share),
                f"section_{step}",
                flops,
                len(pieces) * size,
                4 * MIB,
                in_specs=[vmem] * (len(pieces) + 4),
                out_specs=(vmem, vmem),
            )(*pieces, w_rows, part_of(step, 0, cols)[0], m_mine[step - 1], m_other[step - 1])
            incs.append(inc)
    inc_all = call(
        functools.partial(last_kernel, levels, zs, xs),
        shape((levels, xs, cols, rank_cap), BF16),
        "last_sums",
        flops,
        len(pieces) * size,
        4 * MIB,
        in_specs=[vmem] * (len(pieces) + 2 + len(incs)),
        out_specs=vmem,
    )(*pieces, w_rows, picks, *incs)
    inc = lax.all_to_all(
        inc_all.reshape(levels * xs * cols, rank_cap), ("level", "x"), 0, 0, tiled=True
    )

    tiles = 4 if seg % 64 == 0 else 1
    result = call(
        functools.partial(final_kernel, tiles),
        shape((seg, width), BF16),
        "final",
        2 * seg * rank_cap * width,
        seg * (6 * width + 2 * rank_cap),
        16 * MIB,
        in_specs=[vmem] * 3,
        out_specs=hbm,
        scratch_shapes=[pltpu.VMEM((seg, width), BF16), pltpu.SemaphoreType.DMA((tiles,))],
    )(inc, dr, de)
    return result[None, None]


def solution(mesh):
    levels, blocks = mesh.shape["level"], mesh.shape["blk"]
    xs = x_size(mesh)
    zs = blocks // xs
    split = Mesh(mesh.devices.reshape(levels, zs, xs), ("level", "z", "x"))
    seg = P("level", ("z", "x"))
    return jax.shard_map(
        functools.partial(per_device, zs, xs),
        mesh=split,
        in_specs=(seg, seg, seg, seg, seg, P(), P()),
        out_specs=seg,
        check_vma=False,
    )
```
